32 devices in a mesh: dp: 8 (over y, x, core), tensor: 4 (over z).
Axes of the slice: x: 2, y: 2, z: 4, core: 2. Of those that a mesh axis runs over, the one named last changes fastest.
Arguments:
- activations: bfloat16 [3072, 16384], P(('dp', 'tensor')), may hold values from -6 to 6
- out_grad: bfloat16 [3072, 16384], P('dp', 'tensor'), may hold values from -0.25 to 0.25
- block_ids: int32 [4, 12], replicated, may hold values from 0 to 127, as said below
- owner_map: int32 [8, 4], replicated, may hold values from 0 to 1, as said below
- master: float32 [1024, 16384], P('dp', 'tensor'), may hold values from -3 to 3
- moment: float32 [1024, 16384], P('dp', 'tensor'), may hold values from -3 to 3
- second: float32 [1024, 16384], P('dp', 'tensor'), may hold values from 0.01 to 2
Outputs:
- new_master: float32 [1024, 16384], P('dp', 'tensor')
- new_moment: float32 [1024, 16384], P('dp', 'tensor')
- new_second: float32 [1024, 16384], P('dp', 'tensor')
- hot_weights: bfloat16 [1024, 16384], P('dp')
- cold_recv: float32 [4096, 16384], P('dp', 'tensor')
The draws below stay inside these ranges and needn't reach their ends.
Inputs may be any that keep to these rules, and one draw needn't show every extreme that they name: `block_ids`: the 12 block numbers in a row are distinct. `owner_map`: each row has between 1 and 3 ones; some row has exactly 3 ones and some row exactly 1.
All inputs are finite; a program needn't handle non-finite values.
Results may differ from the reference program's by a relative error of at most 0.006.
Values may be sent and summed in bfloat16 or wider, within the bound.
A program may use at most 128 MiB of HBM per device.

```python
import math
import jax
import jax.numpy as jnp
from jax import lax

D = 16384
QO = 16384
BLOCK = 128
HOT = 8
COLD = 4
MOSTC = 3
TOK = 384
TOKENS = 3072
HOTR = 1024
N_DP = 8
N_TENSOR = 4


def draw_block_ids(key, part):
    keys = jax.random.split(jax.random.fold_in(key, 11), N_TENSOR)
    rows = jax.vmap(lambda single: jax.random.permutation(single, D // BLOCK)[:HOT + COLD])(keys)
    return rows.astype(jnp.int32)


def draw_owner_map(key, part):
    base = jax.random.fold_in(key, 23)
    first, second_key, third = jax.random.split(base, 3)
    counts = jax.random.randint(first, (N_DP,), COLD - MOSTC, MOSTC + 1)
    chosen = jax.random.permutation(second_key, N_DP)
    counts = counts.at[chosen[0]].set(MOSTC).at[chosen[1]].set(COLD - MOSTC)
    ranks = jax.vmap(lambda single: jax.random.permutation(single, COLD))(jax.random.split(third, N_DP))
    return (ranks < counts[:, None]).astype(jnp.int32)


def shard_levels(rng, shape, cuts, low, high):
    loudness, own = 1.0, jax.random.fold_in(rng, 6)
    for position, parts in cuts:
        draws = jnp.exp(jax.random.uniform(jax.random.fold_in(own, position), (parts,), jnp.float32, low / len(cuts), high / len(cuts)))
        loudness = loudness * jnp.repeat(draws, shape[position] // parts).reshape([-1 if axis == position else 1 for axis in range(len(shape))])
    return loudness


def bell_draw(own_key, extent, deviation, limit, shards=(), kind=jnp.bfloat16):
    factor_of = shard_levels(own_key, extent, shards, -0.22, 0.18) if shards else 1.0
    entries = jax.random.normal(own_key, extent, jnp.float32) * deviation * factor_of
    return jnp.minimum(jnp.maximum(entries, -limit), limit).astype(kind)


def setup_inputs(seed: int = 0) -> dict:
    streams_of = jax.random.split(jax.random.key(seed), 8)
    activations = bell_draw(streams_of[0], (TOKENS, D), 1.0, 6.0, ((0, 32),))
    out_grad = bell_draw(streams_of[1], (TOKENS, QO), (1.0 / TOKENS ** 0.5), 0.25, ((0, 8), (1, 4)))
    block_ids = draw_block_ids(jax.random.fold_in(streams_of[7], 71), 0)
    owner_map = draw_owner_map(jax.random.fold_in(streams_of[7], 71), 0)
    master = bell_draw(streams_of[4], (HOTR, QO), 0.5, 3.0, ((0, 8), (1, 4)), jnp.float32)
    moment = bell_draw(streams_of[5], (HOTR, QO), 0.5, 3.0, ((0, 8), (1, 4)), jnp.float32)
    second = jnp.clip(jnp.exp(math.log(2.0) - 5.2983174 * jax.random.uniform(streams_of[6], (HOTR, QO), jnp.float32) ** shard_levels(streams_of[6], (HOTR, QO), ((0, 8), (1, 4)), -0.2, 0.2)), 0.01, 2.0)
    return {"activations": activations, "out_grad": out_grad, "block_ids": block_ids, "owner_map": owner_map, "master": master, "moment": moment, "second": second}


BETA_ONE = 0.9
BETA_TWO = 0.95
ADAM_EPS = 1e-08
LEARN_RATE = 0.01
DECAY = 0.1
CORRECT_ONE = 1.0 - 0.9 ** 10
CORRECT_TWO = 1.0 - 0.95 ** 10

def pick_blocks(tok_rows, block_row):
    shaped = tok_rows.reshape(tok_rows.shape[0], D // BLOCK, BLOCK)
    return shaped[:, block_row, :].reshape(tok_rows.shape[0], block_row.shape[0] * BLOCK)

def reference(activations, out_grad, block_ids, owner_map, master, moment, second):
    qloc = QO // N_TENSOR
    hot_rows = HOT * BLOCK

    def per_index(carry, index):
        tok_rows = lax.dynamic_slice_in_dim(activations, index * TOK, TOK, 0)
        grad_rows = lax.dynamic_slice_in_dim(out_grad, index * TOK, TOK, 0)
        hot_list = []
        cold_list = []
        for group in range(N_TENSOR):
            chosen = pick_blocks(tok_rows, block_ids[group]).astype(jnp.float32)
            grad_cols = grad_rows[:, group * qloc:(group + 1) * qloc].astype(jnp.float32)
            product = jnp.dot(chosen.T, grad_cols, preferred_element_type=jnp.float32)
            hot_list.append(product[:hot_rows].astype(jnp.bfloat16).astype(jnp.float32))
            cold_list.append(product[hot_rows:].astype(jnp.bfloat16))
        return (carry + jnp.stack(hot_list), jnp.stack(cold_list))
    start_sum = jnp.zeros((N_TENSOR, hot_rows, qloc), jnp.float32)
    hot_sum, cold_parts = lax.scan(per_index, start_sum, jnp.arange(N_DP, dtype=jnp.int32))
    grad = hot_sum.transpose(1, 0, 2).reshape(hot_rows, QO)
    cold_parts = cold_parts.reshape(N_DP, N_TENSOR, COLD, BLOCK, qloc)
    from_prev = jnp.roll(cold_parts, 1, axis=0)
    from_next = jnp.roll(cold_parts, -1, axis=0)
    prev_owner = jnp.roll(owner_map, 1, axis=0)[:, None, :, None, None]
    next_owner = jnp.roll(owner_map, -1, axis=0)[:, None, :, None, None]
    total = jnp.where(prev_owner == 1, from_prev.astype(jnp.float32), 0.0)
    total = total + jnp.where(next_owner == 0, from_next.astype(jnp.float32), 0.0)
    cold_recv = total.transpose(0, 2, 3, 1, 4).reshape(N_DP * COLD * BLOCK, QO)
    new_moment = BETA_ONE * moment + (1.0 - BETA_ONE) * grad
    new_second = BETA_TWO * second + (1.0 - BETA_TWO) * grad * grad
    update = new_moment / CORRECT_ONE / (jnp.sqrt(new_second / CORRECT_TWO) + ADAM_EPS)
    new_master = master - LEARN_RATE * (update + DECAY * master)
    hot_weights = new_master.astype(jnp.bfloat16)
    return (new_master, new_moment, new_second, hot_weights, cold_recv)
```

```python
import functools

import jax
import jax.numpy as jnp
from jax import lax
from jax.experimental import pallas as pl
from jax.experimental.pallas import tpu as pltpu
from jax.sharding import PartitionSpec as P

BLOCK = 128
HOT = 8
COLD = 4
MOSTC = 3

BETA_ONE = 0.9
BETA_TWO = 0.95
ADAM_EPS = 1e-08
LEARN_RATE = 0.01
DECAY = 0.1
CORRECT_ONE = 1.0 - 0.9**10
CORRECT_TWO = 1.0 - 0.95**10

CHUNKS = 4
MESH = pl.DeviceIdType.MESH
F32 = jnp.float32
BF16 = jnp.bfloat16


def adam(grad, master, moment, second):
    new_moment = BETA_ONE * moment + (1.0 - BETA_ONE) * grad
    new_second = BETA_TWO * second + (1.0 - BETA_TWO) * grad * grad
    update = new_moment / CORRECT_ONE / (jnp.sqrt(new_second / CORRECT_TWO) + ADAM_EPS)
    return master - LEARN_RATE * (update + DECAY * master), new_moment, new_second


def halvings(n_dp):
    bits = []
    bit = n_dp // 2
    while bit >= 2:
        bits.append(bit)
        bit //= 2
    return bits


def flip(d, bit):
    return d + bit - 2 * bit * ((d // bit) % 2)


def gather_kernel(n_dp, n_t, unit, ids_ref, owner_ref, act, outbox, cold_outbox):
    i = lax.axis_index("dp")
    t = lax.axis_index("tensor")
    peer = flip(i, 1)
    bits = halvings(n_dp)
    half = outbox.shape[4] // unit

    owned = [owner_ref[i, c] for c in range(COLD)]
    ones = owned[0]
    for c in range(1, COLD):
        ones = ones + owned[c]
    place, taken, left = [], 0, ones
    for c in range(COLD):
        place.append(jnp.where(owned[c] == 1, taken, left))
        taken, left = taken + owned[c], left + 1 - owned[c]

    def column(block):
        return act[:, pl.ds(pl.multiple_of(block * BLOCK, BLOCK), BLOCK)]

    def hot_unit(group, d):
        index = (d * unit) // BLOCK
        cols = column(ids_ref[group, index])
        if unit < BLOCK:
            share = BLOCK // unit
            picked = cols[:, :unit]
            for s in range(1, share):
                picked = jnp.where(d % share == s, cols[:, s * unit : (s + 1) * unit], picked)
            cols = picked
        return cols

    for who, base in ((0, i), (1, peer)):
        for part in range(2):
            for k in range(n_t):
                group = (t + k) % n_t
                for u in range(half):
                    r = 2 * (u + half * (1 - part))
                    d = base
                    for b in bits:
                        if r & b:
                            d = flip(d, b)
                    cols = hot_unit(group, d)
                    outbox[who, part, k, :, pl.ds(u * unit, unit)] = cols
    for k in range(n_t):
        group = (t + k) % n_t
        for p in range(COLD):
            block = 0
            for c in range(COLD):
                block = block + jnp.where(place[c] == p, ids_ref[group, HOT + c], 0)
            cold_outbox[k, :, pl.ds(p * BLOCK, BLOCK)] = column(block)


def gather(n_dp, n_t, unit, ids, owner_map, activations):
    rows_tok = activations.shape[0]
    half = max(n_dp // 4, 1)
    smem = pl.BlockSpec(memory_space=pltpu.SMEM)
    vmem = pl.BlockSpec(memory_space=pltpu.VMEM)
    return pl.pallas_call(
        functools.partial(gather_kernel, n_dp, n_t, unit),
        out_shape=(
            jax.ShapeDtypeStruct((2, 2, n_t, rows_tok, half * unit), BF16),
            jax.ShapeDtypeStruct((n_t, rows_tok, COLD * BLOCK), BF16),
        ),
        in_specs=[smem, smem, vmem],
        out_specs=[vmem, vmem],
    )(ids, owner_map, activations)


def exchange_kernel(
    n_dp,
    n_t,
    outbox,
    cold_outbox,
    og_hbm,
    master_hbm,
    moment_hbm,
    second_hbm,
    grad_out,
    hot_out,
    prev_out,
    next_out,
    inbox,
    cold_inbox,
    og,
    lhs,
    cold_lhs,
    acc,
    rs_send,
    rs_recv,
    cold_send,
    master,
    moment,
    second,
    grad,
    hot_send,
    load_sem,
    sel_send_sem,
    sel_recv_sem,
    og_send_sem,
    og_recv_sem,
    rs_send_sem,
    rs_recv_sem,
    cold_send_sem,
    cold_recv_sem,
    hot_send_sem,
    hot_recv_sem,
    out_sem,
):
    i = lax.axis_index("dp")
    t = lax.axis_index("tensor")
    peer = flip(i, 1)
    rows_tok = cold_outbox.shape[1]
    tok, qlocal = og.shape[0] // 2, og.shape[1]
    units = n_dp // 2
    unit = grad.shape[0]
    half = max(units // 2, 1)
    hw = half * unit
    chunk = qlocal // CHUNKS

    loads = [
        pltpu.make_async_copy(og_hbm, og.at[pl.ds(0, tok)], load_sem.at[0]),
        pltpu.make_async_copy(master_hbm, master, load_sem.at[1]),
        pltpu.make_async_copy(moment_hbm, moment, load_sem.at[2]),
        pltpu.make_async_copy(second_hbm, second, load_sem.at[3]),
    ]
    loads[0].start()

    bits = halvings(n_dp)
    nxt, prv = (i + 1) % n_dp, (i + n_dp - 1) % n_dp
    partners = [(flip(i, b), t) for b in bits] + [(nxt, t), (prv, t), (peer, t)]
    for k in range(1, n_t):
        partners += [(i, (t + k) % n_t), (peer, (t + k) % n_t)]
    barrier = pltpu.get_barrier_semaphore()
    for partner in partners:
        pl.semaphore_signal(barrier, inc=1, device_id=partner, device_id_type=MESH)

    mine = pl.ds(t * rows_tok, rows_tok)
    for part in range(2):
        inbox[part, 0, mine, :] = outbox[0, part, 0]
    cold_inbox[mine, :] = cold_outbox[0]

    pl.semaphore_wait(barrier, len(partners))

    def sel_copy(who, part, k):
        return pltpu.make_async_remote_copy(
            src_ref=outbox.at[who, part, k],
            dst_ref=inbox.at[part, who, pl.ds(t * rows_tok, rows_tok)],
            send_sem=sel_send_sem.at[who, part, k],
            recv_sem=sel_recv_sem.at[who, part, k],
            device_id=(i if who == 0 else peer, (t + k) % n_t),
            device_id_type=MESH,
        )

    def cold_sel_copy(k):
        return pltpu.make_async_remote_copy(
            src_ref=cold_outbox.at[k],
            dst_ref=cold_inbox.at[pl.ds(t * rows_tok, rows_tok)],
            send_sem=sel_send_sem.at[0, 2, k],
            recv_sem=sel_recv_sem.at[0, 2, k],
            device_id=(i, (t + k) % n_t),
            device_id_type=MESH,
        )

    sel = {0: [], 1: [], 2: []}
    for part in range(2):
        for k in range(n_t):
            for who in range(2):
                if who or k:
                    sel[part].append(sel_copy(who, part, k))
    for k in range(1, n_t):
        sel[2].append(cold_sel_copy(k))
    og_copy = pltpu.make_async_remote_copy(
        src_ref=og_hbm,
        dst_ref=og.at[pl.ds(tok, tok)],
        send_sem=og_send_sem,
        recv_sem=og_recv_sem,
        device_id=(peer, t),
        device_id_type=MESH,
    )
    for copy in sel[0]:
        copy.start()
    og_copy.start()
    for part in (2, 1):
        for copy in sel[part]:
            copy.start()
    for load in loads[1:]:
        load.start()

    counts = [b // 2 for b in bits]
    offset = [sum(counts[:s]) * unit for s in range(len(bits))]

    def rs_copy(s, q):
        place_ = (pl.ds(offset[s], counts[s] * unit), pl.ds(q * chunk, chunk))
        return pltpu.make_async_remote_copy(
            src_ref=rs_send.at[place_],
            dst_ref=rs_recv.at[place_],
            send_sem=rs_send_sem.at[s, q],
            recv_sem=rs_recv_sem.at[s, q],
            device_id=(flip(i, bits[s]), t),
            device_id_type=MESH,
        )

    tile = min(512, chunk)

    def product(lhs_value_ref, rows, depth, col):
        return jnp.dot(
            lhs_value_ref[rows, :],
            og[pl.ds(0, depth), pl.ds(col, tile)],
            preferred_element_type=F32,
        )

    def wait_sel(part):
        for copy in sel[part]:
            copy.wait_recv()

    wait_sel(0)
    lhs[0, :, pl.ds(0, tok)] = inbox[0, 0].T
    lhs[0, :, pl.ds(tok, tok)] = inbox[0, 1].T
    loads[0].wait()
    og_copy.wait_recv()
    for q in range(CHUNKS):

        @pl.loop(0, chunk // tile)
        def _(n):
            col = pl.multiple_of(q * chunk + n * tile, tile)
            rs_send[pl.ds(0, hw), pl.ds(col, tile)] = product(
                lhs.at[0], slice(None), 2 * tok, col
            ).astype(BF16)

        rs_copy(0, q).start()

    def cold_copy(p, ahead, q):
        slot = p if ahead else p - 1
        place_ = (slot, slice(None), pl.ds(q * chunk, chunk))
        which = 0 if ahead else 1
        return pltpu.make_async_remote_copy(
            src_ref=cold_send.at[p, :, pl.ds(q * chunk, chunk)],
            dst_ref=(prev_out if ahead else next_out).at[place_],
            send_sem=cold_send_sem.at[which, slot, q],
            recv_sem=cold_recv_sem.at[which, slot, q],
            device_id=(nxt if ahead else prv, t),
            device_id_type=MESH,
        )

    wait_sel(2)
    cold_lhs[...] = cold_inbox[...].T
    for q in range(CHUNKS):

        @pl.loop(0, chunk // tile)
        def _(n):
            col = pl.multiple_of(q * chunk + n * tile, tile)
            out = product(cold_lhs, slice(None), tok, col).astype(BF16)
            for p in range(COLD):
                cold_send[p, :, pl.ds(col, tile)] = out[p * BLOCK : (p + 1) * BLOCK]

    def send_cold(q):
        for slot in range(MOSTC):
            cold_copy(slot, True, q).start()
            cold_copy(slot + COLD - MOSTC, False, q).start()

    send_cold(0)
    wait_sel(1)
    lhs[1, :, pl.ds(0, tok)] = inbox[1, 0].T
    lhs[1, :, pl.ds(tok, tok)] = inbox[1, 1].T

    @pl.loop(0, qlocal // tile)
    def _(n):
        col = pl.multiple_of(n * tile, tile)
        acc[:, pl.ds(col, tile)] = product(lhs.at[1], slice(None), 2 * tok, col)

    for load in loads[1:]:
        load.wait()

    def hot_copy(k, q):
        return pltpu.make_async_remote_copy(
            src_ref=hot_send.at[:, pl.ds(q * chunk, chunk)],
            dst_ref=hot_out.at[:, pl.ds(t * qlocal + q * chunk, chunk)],
            send_sem=hot_send_sem.at[k, q],
            recv_sem=hot_recv_sem.at[k, q],
            device_id=(i, (t + k) % n_t),
            device_id_type=MESH,
        )

    def grad_store(q):
        cols = pl.ds(q * chunk, chunk)
        return pltpu.make_async_copy(grad.at[:, cols], grad_out.at[:, cols], out_sem.at[0, q])

    def hot_store(q):
        return pltpu.make_async_copy(
            hot_send.at[:, pl.ds(q * chunk, chunk)],
            hot_out.at[:, pl.ds(t * qlocal + q * chunk, chunk)],
            out_sem.at[1, q],
        )

    step = min(256, chunk)

    def settle(s, q):
        rs_copy(s, q).wait_recv()
        last = s == len(bits) - 1

        @pl.loop(0, chunk // step)
        def _(n):
            cols = pl.ds(pl.multiple_of(q * chunk + n * step, step), step)
            keep = counts[s] * unit
            got = rs_recv[pl.ds(offset[s], keep), cols].astype(F32)
            total = acc[pl.ds(0, keep), cols] + got
            if last:
                grad[:, cols] = total
                new_master, _, _ = adam(total, master[:, cols], moment[:, cols], second[:, cols])
                hot_send[:, cols] = new_master.astype(BF16)
            else:
                sent = counts[s + 1] * unit
                acc[pl.ds(0, sent), cols] = total[:sent]
                rs_send[pl.ds(offset[s + 1], sent), cols] = total[sent:].astype(BF16)

        if last:
            for k in range(1, n_t):
                hot_copy(k, q).start()
            grad_store(q).start()
            hot_store(q).start()
        else:
            rs_copy(s + 1, q).start()

    cold_sent = 1
    for wave in range(CHUNKS + len(bits) - 1):
        for s in reversed(range(len(bits))):
            q = wave - s
            if 0 <= q < CHUNKS:
                settle(s, q)
        if cold_sent < CHUNKS:
            send_cold(cold_sent)
            cold_sent += 1

    for part in range(3):
        for copy in sel[part]:
            copy.wait_send()
    og_copy.wait_send()
    for q in range(CHUNKS):
        for s in range(len(bits)):
            rs_copy(s, q).wait_send()
        grad_store(q).wait()
        hot_store(q).wait()
        for k in range(1, n_t):
            hot_copy(k, q).wait()
        for slot in range(MOSTC):
            cold_copy(slot, True, q).wait()
            cold_copy(slot + COLD - MOSTC, False, q).wait()


def exchange(n_dp, n_t, outbox, cold_outbox, out_grad, master, moment, second):
    tok, qlocal = out_grad.shape
    unit = master.shape[0]
    units = n_dp // 2
    half = max(units // 2, 1)
    stages = max(n_dp.bit_length() - 2, 1)
    traded = (units - 1) * unit
    vmem = pl.BlockSpec(memory_space=pltpu.VMEM)
    anywhere = pl.BlockSpec(memory_space=pl.ANY)
    dma = pltpu.SemaphoreType.DMA
    return pl.pallas_call(
        functools.partial(exchange_kernel, n_dp, n_t),
        out_shape=(
            jax.ShapeDtypeStruct((unit, qlocal), F32),
            jax.ShapeDtypeStruct((unit, qlocal * n_t), BF16),
            jax.ShapeDtypeStruct((MOSTC, BLOCK, qlocal), BF16),
            jax.ShapeDtypeStruct((MOSTC, BLOCK, qlocal), BF16),
        ),
        in_specs=[vmem, vmem] + [anywhere] * 4,
        out_specs=[anywhere] * 4,
        scratch_shapes=[
            pltpu.VMEM((2, 2, tok, half * unit), BF16),
            pltpu.VMEM((tok, COLD * BLOCK), BF16),
            pltpu.VMEM((2 * tok, qlocal), BF16),
            pltpu.VMEM((2, half * unit, 2 * tok), BF16),
            pltpu.VMEM((COLD * BLOCK, tok), BF16),
            pltpu.VMEM((half * unit, qlocal), F32),
            pltpu.VMEM((traded, qlocal), BF16),
            pltpu.VMEM((traded, qlocal), BF16),
            pltpu.VMEM((COLD, BLOCK, qlocal), BF16),
            pltpu.VMEM((unit, qlocal), F32),
            pltpu.VMEM((unit, qlocal), F32),
            pltpu.VMEM((unit, qlocal), F32),
            pltpu.VMEM((unit, qlocal), F32),
            pltpu.VMEM((unit, qlocal), BF16),
            dma((4,)),
            dma((2, 3, n_t)),
            dma((2, 3, n_t)),
            dma(()),
            dma(()),
            dma((stages, CHUNKS)),
            dma((stages, CHUNKS)),
            dma((2, MOSTC, CHUNKS)),
            dma((2, MOSTC, CHUNKS)),
            dma((n_t, CHUNKS)),
            dma((n_t, CHUNKS)),
            dma((2, CHUNKS)),
        ],
        compiler_params=pltpu.CompilerParams(
            collective_id=0, has_side_effects=True, vmem_limit_bytes=60 * 1024 * 1024
        ),
    )(outbox, cold_outbox, out_grad, master, moment, second)


def cold_kernel(where_ref, owner_ref, prev_ref, next_ref, out_ref):
    c = pl.program_id(0)
    from_prev = owner_ref[where_ref[0], c] == 1
    from_next = owner_ref[where_ref[1], c] == 0
    total = jnp.where(from_prev, prev_ref[0].astype(F32), 0.0)
    out_ref[...] = total + jnp.where(from_next, next_ref[0].astype(F32), 0.0)


def ones_before(owner_ref, row, c):
    count = 0
    for b in range(COLD):
        count = count + jnp.where(b < c, owner_ref[row, b], 0)
    return count


def prev_slot(c, n, where_ref, owner_ref):
    return jnp.minimum(ones_before(owner_ref, where_ref[0], c), MOSTC - 1), 0, n


def next_slot(c, n, where_ref, owner_ref):
    row = where_ref[1]
    ones = ones_before(owner_ref, row, COLD)
    place = ones + c - ones_before(owner_ref, row, c)
    return jnp.clip(place - (COLD - MOSTC), 0, MOSTC - 1), 0, n


def merge_cold(where, owner_map, from_prev, from_next):
    qlocal = from_prev.shape[2]
    width = qlocal // 2
    return pl.pallas_call(
        cold_kernel,
        out_shape=jax.ShapeDtypeStruct((COLD * BLOCK, qlocal), F32),
        grid_spec=pltpu.PrefetchScalarGridSpec(
            num_scalar_prefetch=2,
            grid=(COLD, 2),
            in_specs=[
                pl.BlockSpec((1, BLOCK, width), prev_slot),
                pl.BlockSpec((1, BLOCK, width), next_slot),
            ],
            out_specs=pl.BlockSpec((BLOCK, width), lambda c, n, *_: (c, n)),
        ),
    )(where, owner_map, from_prev, from_next)


def per_device(n_dp, n_t, activations, out_grad, block_ids, owner_map, master, moment, second):
    outbox, cold_outbox = gather(n_dp, n_t, master.shape[0], block_ids, owner_map, activations)
    grad, hot_weights, from_prev, from_next = exchange(
        n_dp, n_t, outbox, cold_outbox, out_grad, master, moment, second
    )
    index = lax.axis_index("dp")
    where = jnp.stack([(index + n_dp - 1) % n_dp, (index + 1) % n_dp]).astype(jnp.int32)
    cold_recv = merge_cold(where, owner_map, from_prev, from_next)
    new_master, new_moment, new_second = adam(grad, master, moment, second)
    return (new_master, new_moment, new_second, hot_weights, cold_recv)


def solution(mesh):
    return jax.shard_map(
        functools.partial(per_device, mesh.shape["dp"], mesh.shape["tensor"]),
        mesh=mesh,
        in_specs=(
            P(("dp", "tensor"), None),
            P("dp", "tensor"),
            P(),
            P(),
            P("dp", "tensor"),
            P("dp", "tensor"),
            P("dp", "tensor"),
        ),
        out_specs=(
            P("dp", "tensor"),
            P("dp", "tensor"),
            P("dp", "tensor"),
            P("dp", None),
            P("dp", "tensor"),
        ),
        check_vma=False,
    )
```

```python
import functools

import jax
import jax.numpy as jnp
from jax import lax
from jax.experimental import pallas as pl
from jax.experimental.pallas import tpu as pltpu
from jax.sharding import PartitionSpec as P

BLOCK = 128
HOT = 8
COLD = 4
MOSTC = 3

BETA_ONE = 0.9
BETA_TWO = 0.95
ADAM_EPS = 1e-08
LEARN_RATE = 0.01
DECAY = 0.1
CORRECT_ONE = 1.0 - 0.9**10
CORRECT_TWO = 1.0 - 0.95**10

CHUNKS = 4
MESH = pl.DeviceIdType.MESH
F32 = jnp.float32
BF16 = jnp.bfloat16


def adam(grad, master, moment, second):
    new_moment = BETA_ONE * moment + (1.0 - BETA_ONE) * grad
    new_second = BETA_TWO * second + (1.0 - BETA_TWO) * grad * grad
    update = new_moment / CORRECT_ONE / (jnp.sqrt(new_second / CORRECT_TWO) + ADAM_EPS)
    return master - LEARN_RATE * (update + DECAY * master), new_moment, new_second


def halvings(n_dp):
    bits = []
    bit = n_dp // 2
    while bit >= 2:
        bits.append(bit)
        bit //= 2
    return bits


def flip(d, bit):
    return d + bit - 2 * bit * ((d // bit) % 2)


def gather_kernel(n_dp, n_t, unit, ids_ref, owner_ref, act, outbox, cold_outbox):
    i = lax.axis_index("dp")
    t = lax.axis_index("tensor")
    peer = flip(i, 1)
    bits = halvings(n_dp)
    half = outbox.shape[4] // unit

    owned = [owner_ref[i, c] for c in range(COLD)]
    ones = owned[0]
    for c in range(1, COLD):
        ones = ones + owned[c]
    place, taken, left = [], 0, ones
    for c in range(COLD):
        place.append(jnp.where(owned[c] == 1, taken, left))
        taken, left = taken + owned[c], left + 1 - owned[c]

    def column(block):
        return act[:, pl.ds(pl.multiple_of(block * BLOCK, BLOCK), BLOCK)]

    def hot_unit(group, d):
        index = (d * unit) // BLOCK
        cols = column(ids_ref[group, index])
        if unit < BLOCK:
            share = BLOCK // unit
            picked = cols[:, :unit]
            for s in range(1, share):
                picked = jnp.where(d % share == s, cols[:, s * unit : (s + 1) * unit], picked)
            cols = picked
        return cols

    for who, base in ((0, i), (1, peer)):
        for part in range(2):
            for k in range(n_t):
                group = (t + k) % n_t
                for u in range(half):
                    r = 2 * (u + half * (1 - part))
                    d = base
                    for b in bits:
                        if r & b:
                            d = flip(d, b)
                    cols = hot_unit(group, d)
                    outbox[who, part, k, :, pl.ds(u * unit, unit)] = cols
    for k in range(n_t):
        group = (t + k) % n_t
        for p in range(COLD):
            block = 0
            for c in range(COLD):
                block = block + jnp.where(place[c] == p, ids_ref[group, HOT + c], 0)
            cold_outbox[k, :, pl.ds(p * BLOCK, BLOCK)] = column(block)


def gather(n_dp, n_t, unit, ids, owner_map, activations):
    rows_tok = activations.shape[0]
    half = max(n_dp // 4, 1)
    smem = pl.BlockSpec(memory_space=pltpu.SMEM)
    vmem = pl.BlockSpec(memory_space=pltpu.VMEM)
    return pl.pallas_call(
        functools.partial(gather_kernel, n_dp, n_t, unit),
        out_shape=(
            jax.ShapeDtypeStruct((2, 2, n_t, rows_tok, half * unit), BF16),
            jax.ShapeDtypeStruct((n_t, rows_tok, COLD * BLOCK), BF16),
        ),
        in_specs=[smem, smem, vmem],
        out_specs=[vmem, vmem],
    )(ids, owner_map, activations)


def exchange_kernel(
    n_dp,
    n_t,
    outbox,
    cold_outbox,
    og_hbm,
    master_hbm,
    moment_hbm,
    second_hbm,
    grad_out,
    hot_out,
    prev_out,
    next_out,
    inbox,
    cold_inbox,
    og,
    lhs,
    cold_lhs,
    acc,
    rs_send,
    rs_recv,
    cold_send,
    master,
    moment,
    second,
    grad,
    hot_send,
    load_sem,
    sel_send_sem,
    sel_recv_sem,
    og_send_sem,
    og_recv_sem,
    rs_send_sem,
    rs_recv_sem,
    cold_send_sem,
    cold_recv_sem,
    hot_send_sem,
    hot_recv_sem,
    out_sem,
):
    i = lax.axis_index("dp")
    t = lax.axis_index("tensor")
    peer = flip(i, 1)
    rows_tok = cold_outbox.shape[1]
    tok, qlocal = og.shape[0] // 2, og.shape[1]
    units = n_dp // 2
    unit = grad.shape[0]
    half = max(units // 2, 1)
    hw = half * unit
    chunk = qlocal // CHUNKS

    loads = [
        pltpu.make_async_copy(og_hbm, og.at[pl.ds(0, tok)], load_sem.at[0]),
        pltpu.make_async_copy(master_hbm, master, load_sem.at[1]),
        pltpu.make_async_copy(moment_hbm, moment, load_sem.at[2]),
        pltpu.make_async_copy(second_hbm, second, load_sem.at[3]),
    ]
    loads[0].start()

    bits = halvings(n_dp)
    nxt, prv = (i + 1) % n_dp, (i + n_dp - 1) % n_dp
    partners = [(flip(i, b), t) for b in bits] + [(nxt, t), (prv, t), (peer, t)]
    for k in range(1, n_t):
        partners += [(i, (t + k) % n_t), (peer, (t + k) % n_t)]
    barrier = pltpu.get_barrier_semaphore()
    for partner in partners:
        pl.semaphore_signal(barrier, inc=1, device_id=partner, device_id_type=MESH)

    mine = pl.ds(t * rows_tok, rows_tok)
    for part in range(2):
        inbox[part, 0, mine, :] = outbox[0, part, 0]
    cold_inbox[mine, :] = cold_outbox[0]

    pl.semaphore_wait(barrier, len(partners))

    def sel_copy(who, part, k):
        return pltpu.make_async_remote_copy(
            src_ref=outbox.at[who, part, k],
            dst_ref=inbox.at[part, who, pl.ds(t * rows_tok, rows_tok)],
            send_sem=sel_send_sem.at[who, part, k],
            recv_sem=sel_recv_sem.at[who, part, k],
            device_id=(i if who == 0 else peer, (t + k) % n_t),
            device_id_type=MESH,
        )

    def cold_sel_copy(k):
        return pltpu.make_async_remote_copy(
            src_ref=cold_outbox.at[k],
            dst_ref=cold_inbox.at[pl.ds(t * rows_tok, rows_tok)],
            send_sem=sel_send_sem.at[0, 2, k],
            recv_sem=sel_recv_sem.at[0, 2, k],
            device_id=(i, (t + k) % n_t),
            device_id_type=MESH,
        )

    sel = {0: [], 1: [], 2: []}
    for part in range(2):
        for k in range(n_t):
            for who in range(2):
                if who or k:
                    sel[part].append(sel_copy(who, part, k))
    for k in range(1, n_t):
        sel[2].append(cold_sel_copy(k))
    og_copy = pltpu.make_async_remote_copy(
        src_ref=og_hbm,
        dst_ref=og.at[pl.ds(tok, tok)],
        send_sem=og_send_sem,
        recv_sem=og_recv_sem,
        device_id=(peer, t),
        device_id_type=MESH,
    )
    og_copy.start()
    for part in (2, 0, 1):
        for copy in sel[part]:
            copy.start()
    for load in loads[1:]:
        load.start()

    counts = [b // 2 for b in bits]
    offset = [sum(counts[:s]) * unit for s in range(len(bits))]

    def rs_copy(s, q):
        place_ = (pl.ds(offset[s], counts[s] * unit), pl.ds(q * chunk, chunk))
        return pltpu.make_async_remote_copy(
            src_ref=rs_send.at[place_],
            dst_ref=rs_recv.at[place_],
            send_sem=rs_send_sem.at[s, q],
            recv_sem=rs_recv_sem.at[s, q],
            device_id=(flip(i, bits[s]), t),
            device_id_type=MESH,
        )

    tile = min(512, chunk)

    def product(lhs_value_ref, rows, depth, col):
        return jnp.dot(
            lhs_value_ref[rows, :],
            og[pl.ds(0, depth), pl.ds(col, tile)],
            preferred_element_type=F32,
        )

    def wait_sel(part):
        for copy in sel[part]:
            copy.wait_recv()

    def cold_copy(p, ahead, q):
        slot = p if ahead else p - 1
        place_ = (slot, slice(None), pl.ds(q * chunk, chunk))
        which = 0 if ahead else 1
        return pltpu.make_async_remote_copy(
            src_ref=cold_send.at[p, :, pl.ds(q * chunk, chunk)],
            dst_ref=(prev_out if ahead else next_out).at[place_],
            send_sem=cold_send_sem.at[which, slot, q],
            recv_sem=cold_recv_sem.at[which, slot, q],
            device_id=(nxt if ahead else prv, t),
            device_id_type=MESH,
        )

    wait_sel(2)
    cold_lhs[...] = cold_inbox[...].T
    loads[0].wait()
    for q in range(CHUNKS):

        @pl.loop(0, chunk // tile)
        def _(n):
            col = pl.multiple_of(q * chunk + n * tile, tile)
            out = product(cold_lhs, slice(None), tok, col).astype(BF16)
            for p in range(COLD):
                cold_send[p, :, pl.ds(col, tile)] = out[p * BLOCK : (p + 1) * BLOCK]

    def send_cold(q):
        for slot in range(MOSTC):
            cold_copy(slot, True, q).start()
            cold_copy(slot + COLD - MOSTC, False, q).start()

    direct = (i % 4 == 1) | (i % 4 == 2)
    send_cold(0)
    wait_sel(0)
    lhs[0, :, pl.ds(0, tok)] = inbox[0, 0].T
    lhs[0, :, pl.ds(tok, tok)] = inbox[0, 1].T
    og_copy.wait_recv()
    for q in range(CHUNKS):

        @pl.loop(0, chunk // tile)
        def _(n):
            col = pl.multiple_of(q * chunk + n * tile, tile)
            rs_send[pl.ds(0, hw), pl.ds(col, tile)] = product(
                lhs.at[0], slice(None), 2 * tok, col
            ).astype(BF16)

        rs_copy(0, q).start()

    @pl.when(direct)
    def _():
        send_cold(1)

    wait_sel(1)
    lhs[1, :, pl.ds(0, tok)] = inbox[1, 0].T
    lhs[1, :, pl.ds(tok, tok)] = inbox[1, 1].T

    @pl.loop(0, qlocal // tile)
    def _(n):
        col = pl.multiple_of(n * tile, tile)
        acc[:, pl.ds(col, tile)] = product(lhs.at[1], slice(None), 2 * tok, col)

    for load in loads[1:]:
        load.wait()

    def hot_copy(way, hop, q):
        origin = t - hop if way == 0 else t + hop
        cols = pl.ds(q * chunk, chunk)
        place_ = (slice(None), pl.ds(origin * qlocal + q * chunk, chunk))
        return pltpu.make_async_remote_copy(
            src_ref=hot_send.at[:, cols] if hop == 0 else hot_out.at[place_],
            dst_ref=hot_out.at[place_],
            send_sem=hot_send_sem.at[way, hop, q],
            recv_sem=hot_recv_sem.at[way, hop, q],
            device_id=(i, (t + 1) % n_t if way == 0 else (t + n_t - 1) % n_t),
            device_id_type=MESH,
        )

    def can_send(way, hop):
        if way == 0:
            return (t >= hop) & (t < n_t - 1)
        return (t + hop <= n_t - 1) & (t > 0)

    def send_hot(hop, q):
        for way in range(2):

            @pl.when(can_send(way, hop))
            def _():
                if hop:
                    hot_copy(way, hop - 1, q).wait_recv()
                hot_copy(way, hop, q).start()

    def grad_store(q):
        cols = pl.ds(q * chunk, chunk)
        return pltpu.make_async_copy(grad.at[:, cols], grad_out.at[:, cols], out_sem.at[0, q])

    def hot_store(q):
        return pltpu.make_async_copy(
            hot_send.at[:, pl.ds(q * chunk, chunk)],
            hot_out.at[:, pl.ds(t * qlocal + q * chunk, chunk)],
            out_sem.at[1, q],
        )

    step = min(256, chunk)

    def settle(s, q):
        rs_copy(s, q).wait_recv()
        last = s == len(bits) - 1

        @pl.loop(0, chunk // step)
        def _(n):
            cols = pl.ds(pl.multiple_of(q * chunk + n * step, step), step)
            keep = counts[s] * unit
            got = rs_recv[pl.ds(offset[s], keep), cols].astype(F32)
            total = acc[pl.ds(0, keep), cols] + got
            if last:
                grad[:, cols] = total
                new_master, _, _ = adam(total, master[:, cols], moment[:, cols], second[:, cols])
                hot_send[:, cols] = new_master.astype(BF16)
            else:
                sent = counts[s + 1] * unit
                acc[pl.ds(0, sent), cols] = total[:sent]
                rs_send[pl.ds(offset[s + 1], sent), cols] = total[sent:].astype(BF16)

        if last:
            send_hot(0, q)
            grad_store(q).start()
            hot_store(q).start()
        else:
            rs_copy(s + 1, q).start()

    for wave in range(CHUNKS + len(bits) - 1 + n_t - 2):
        for s in reversed(range(len(bits))):
            q = wave - s
            if 0 <= q < CHUNKS:
                settle(s, q)
        if 1 <= wave < CHUNKS:

            @pl.when(jnp.logical_not(direct))
            def _():
                send_cold(wave)

        if 1 <= wave < CHUNKS - 1:

            @pl.when(direct)
            def _():
                send_cold(wave + 1)

        for hop in range(1, n_t - 1):
            q = wave - (len(bits) - 1) - hop
            if 0 <= q < CHUNKS:
                send_hot(hop, q)

    for part in range(3):
        for copy in sel[part]:
            copy.wait_send()
    og_copy.wait_send()
    for q in range(CHUNKS):
        for s in range(len(bits)):
            rs_copy(s, q).wait_send()
        grad_store(q).wait()
        hot_store(q).wait()
        for hop in range(n_t - 1):
            for way in range(2):

                @pl.when(can_send(way, hop))
                def _():
                    hot_copy(way, hop, q).wait_send()

                @pl.when((t == n_t - 1) if way == 0 else (t == 0))
                def _():
                    hot_copy(way, hop, q).wait_recv()

        for slot in range(MOSTC):
            cold_copy(slot, True, q).wait()
            cold_copy(slot + COLD - MOSTC, False, q).wait()


def exchange(n_dp, n_t, outbox, cold_outbox, out_grad, master, moment, second):
    tok, qlocal = out_grad.shape
    unit = master.shape[0]
    units = n_dp // 2
    half = max(units // 2, 1)
    stages = max(n_dp.bit_length() - 2, 1)
    traded = (units - 1) * unit
    vmem = pl.BlockSpec(memory_space=pltpu.VMEM)
    anywhere = pl.BlockSpec(memory_space=pl.ANY)
    dma = pltpu.SemaphoreType.DMA
    return pl.pallas_call(
        functools.partial(exchange_kernel, n_dp, n_t),
        out_shape=(
            jax.ShapeDtypeStruct((unit, qlocal), F32),
            jax.ShapeDtypeStruct((unit, qlocal * n_t), BF16),
            jax.ShapeDtypeStruct((MOSTC, BLOCK, qlocal), BF16),
            jax.ShapeDtypeStruct((MOSTC, BLOCK, qlocal), BF16),
        ),
        in_specs=[vmem, vmem] + [anywhere] * 4,
        out_specs=[anywhere] * 4,
        scratch_shapes=[
            pltpu.VMEM((2, 2, tok, half * unit), BF16),
            pltpu.VMEM((tok, COLD * BLOCK), BF16),
            pltpu.VMEM((2 * tok, qlocal), BF16),
            pltpu.VMEM((2, half * unit, 2 * tok), BF16),
            pltpu.VMEM((COLD * BLOCK, tok), BF16),
            pltpu.VMEM((half * unit, qlocal), F32),
            pltpu.VMEM((traded, qlocal), BF16),
            pltpu.VMEM((traded, qlocal), BF16),
            pltpu.VMEM((COLD, BLOCK, qlocal), BF16),
            pltpu.VMEM((unit, qlocal), F32),
            pltpu.VMEM((unit, qlocal), F32),
            pltpu.VMEM((unit, qlocal), F32),
            pltpu.VMEM((unit, qlocal), F32),
            pltpu.VMEM((unit, qlocal), BF16),
            dma((4,)),
            dma((2, 3, n_t)),
            dma((2, 3, n_t)),
            dma(()),
            dma(()),
            dma((stages, CHUNKS)),
            dma((stages, CHUNKS)),
            dma((2, MOSTC, CHUNKS)),
            dma((2, MOSTC, CHUNKS)),
            dma((2, n_t, CHUNKS)),
            dma((2, n_t, CHUNKS)),
            dma((2, CHUNKS)),
        ],
        compiler_params=pltpu.CompilerParams(
            collective_id=0, has_side_effects=True, vmem_limit_bytes=60 * 1024 * 1024
        ),
    )(outbox, cold_outbox, out_grad, master, moment, second)


def cold_kernel(where_ref, owner_ref, prev_ref, next_ref, out_ref):
    c = pl.program_id(0)
    from_prev = owner_ref[where_ref[0], c] == 1
    from_next = owner_ref[where_ref[1], c] == 0
    total = jnp.where(from_prev, prev_ref[0].astype(F32), 0.0)
    out_ref[...] = total + jnp.where(from_next, next_ref[0].astype(F32), 0.0)


def ones_before(owner_ref, row, c):
    count = 0
    for b in range(COLD):
        count = count + jnp.where(b < c, owner_ref[row, b], 0)
    return count


def prev_slot(c, n, where_ref, owner_ref):
    return jnp.minimum(ones_before(owner_ref, where_ref[0], c), MOSTC - 1), 0, n


def next_slot(c, n, where_ref, owner_ref):
    row = where_ref[1]
    ones = ones_before(owner_ref, row, COLD)
    place = ones + c - ones_before(owner_ref, row, c)
    return jnp.clip(place - (COLD - MOSTC), 0, MOSTC - 1), 0, n


def merge_cold(where, owner_map, from_prev, from_next):
    qlocal = from_prev.shape[2]
    width = qlocal // 4
    return pl.pallas_call(
        cold_kernel,
        out_shape=jax.ShapeDtypeStruct((COLD * BLOCK, qlocal), F32),
        grid_spec=pltpu.PrefetchScalarGridSpec(
            num_scalar_prefetch=2,
            grid=(COLD, 4),
            in_specs=[
                pl.BlockSpec((1, BLOCK, width), prev_slot),
                pl.BlockSpec((1, BLOCK, width), next_slot),
            ],
            out_specs=pl.BlockSpec((BLOCK, width), lambda c, n, *_: (c, n)),
        ),
    )(where, owner_map, from_prev, from_next)


def per_device(n_dp, n_t, activations, out_grad, block_ids, owner_map, master, moment, second):
    outbox, cold_outbox = gather(n_dp, n_t, master.shape[0], block_ids, owner_map, activations)
    grad, hot_weights, from_prev, from_next = exchange(
        n_dp, n_t, outbox, cold_outbox, out_grad, master, moment, second
    )
    index = lax.axis_index("dp")
    where = jnp.stack([(index + n_dp - 1) % n_dp, (index + 1) % n_dp]).astype(jnp.int32)
    cold_recv = merge_cold(where, owner_map, from_prev, from_next)
    new_master, new_moment, new_second = adam(grad, master, moment, second)
    return (new_master, new_moment, new_second, hot_weights, cold_recv)


def solution(mesh):
    return jax.shard_map(
        functools.partial(per_device, mesh.shape["dp"], mesh.shape["tensor"]),
        mesh=mesh,
        in_specs=(
            P(("dp", "tensor"), None),
            P("dp", "tensor"),
            P(),
            P(),
            P("dp", "tensor"),
            P("dp", "tensor"),
            P("dp", "tensor"),
        ),
        out_specs=(
            P("dp", "tensor"),
            P("dp", "tensor"),
            P("dp", "tensor"),
            P("dp", None),
            P("dp", "tensor"),
        ),
        check_vma=False,
    )
```

```python
import functools

import jax
import jax.numpy as jnp
from jax import lax
from jax.experimental import pallas as pl
from jax.experimental.pallas import tpu as pltpu
from jax.sharding import PartitionSpec as P

BLOCK = 128
HOT = 8
COLD = 4
MOSTC = 3

BETA_ONE = 0.9
BETA_TWO = 0.95
ADAM_EPS = 1e-08
LEARN_RATE = 0.01
DECAY = 0.1
CORRECT_ONE = 1.0 - 0.9**10
CORRECT_TWO = 1.0 - 0.95**10

CHUNKS = 8
MESH = pl.DeviceIdType.MESH
F32 = jnp.float32
BF16 = jnp.bfloat16


def adam(grad, master, moment, second):
    new_moment = BETA_ONE * moment + (1.0 - BETA_ONE) * grad
    new_second = BETA_TWO * second + (1.0 - BETA_TWO) * grad * grad
    update = new_moment / CORRECT_ONE / (jnp.sqrt(new_second / CORRECT_TWO) + ADAM_EPS)
    return master - LEARN_RATE * (update + DECAY * master), new_moment, new_second


def halvings(n_dp):
    bits = []
    bit = n_dp // 2
    while bit >= 2:
        bits.append(bit)
        bit //= 2
    return bits


def flip(d, bit):
    return d + bit - 2 * bit * ((d // bit) % 2)


def gather_kernel(n_dp, n_t, unit, ids_ref, owner_ref, act, outbox, cold_outbox):
    i = lax.axis_index("dp")
    t = lax.axis_index("tensor")
    peer = flip(i, 1)
    bits = halvings(n_dp)
    half = outbox.shape[4] // unit

    owned = [owner_ref[i, c] for c in range(COLD)]
    ones = owned[0]
    for c in range(1, COLD):
        ones = ones + owned[c]
    place, taken, left = [], 0, ones
    for c in range(COLD):
        place.append(jnp.where(owned[c] == 1, taken, left))
        taken, left = taken + owned[c], left + 1 - owned[c]

    def column(block):
        return act[:, pl.ds(pl.multiple_of(block * BLOCK, BLOCK), BLOCK)]

    def hot_unit(group, d):
        index = (d * unit) // BLOCK
        cols = column(ids_ref[group, index])
        if unit < BLOCK:
            share = BLOCK // unit
            picked = cols[:, :unit]
            for s in range(1, share):
                picked = jnp.where(d % share == s, cols[:, s * unit : (s + 1) * unit], picked)
            cols = picked
        return cols

    for who, base in ((0, i), (1, peer)):
        for part in range(2):
            for k in range(n_t):
                group = (t + k) % n_t
                for u in range(half):
                    r = 2 * (u + half * (1 - part))
                    d = base
                    for b in bits:
                        if r & b:
                            d = flip(d, b)
                    cols = hot_unit(group, d)
                    outbox[who, part, k, :, pl.ds(u * unit, unit)] = cols
    for k in range(n_t):
        group = (t + k) % n_t
        for p in range(COLD):
            block = 0
            for c in range(COLD):
                block = block + jnp.where(place[c] == p, ids_ref[group, HOT + c], 0)
            cold_outbox[k, :, pl.ds(p * BLOCK, BLOCK)] = column(block)


def gather(n_dp, n_t, unit, ids, owner_map, activations):
    rows_tok = activations.shape[0]
    half = max(n_dp // 4, 1)
    smem = pl.BlockSpec(memory_space=pltpu.SMEM)
    vmem = pl.BlockSpec(memory_space=pltpu.VMEM)
    return pl.pallas_call(
        functools.partial(gather_kernel, n_dp, n_t, unit),
        out_shape=(
            jax.ShapeDtypeStruct((2, 2, n_t, rows_tok, half * unit), BF16),
            jax.ShapeDtypeStruct((n_t, rows_tok, COLD * BLOCK), BF16),
        ),
        in_specs=[smem, smem, vmem],
        out_specs=[vmem, vmem],
    )(ids, owner_map, activations)


def exchange_kernel(
    n_dp,
    n_t,
    outbox,
    cold_outbox,
    og_hbm,
    master_hbm,
    moment_hbm,
    second_hbm,
    grad_out,
    hot_out,
    prev_out,
    next_out,
    inbox,
    cold_inbox,
    og,
    lhs,
    cold_lhs,
    acc,
    rs_send,
    rs_recv,
    cold_send,
    master,
    moment,
    second,
    grad,
    hot_send,
    load_sem,
    sel_send_sem,
    sel_recv_sem,
    og_send_sem,
    og_recv_sem,
    rs_send_sem,
    rs_recv_sem,
    cold_send_sem,
    cold_recv_sem,
    hot_send_sem,
    hot_recv_sem,
    out_sem,
):
    i = lax.axis_index("dp")
    t = lax.axis_index("tensor")
    peer = flip(i, 1)
    rows_tok = cold_outbox.shape[1]
    tok, qlocal = og.shape[0] // 2, og.shape[1]
    units = n_dp // 2
    unit = grad.shape[0]
    half = max(units // 2, 1)
    hw = half * unit
    chunk = qlocal // CHUNKS

    loads = [
        pltpu.make_async_copy(og_hbm, og.at[pl.ds(0, tok)], load_sem.at[0]),
        pltpu.make_async_copy(master_hbm, master, load_sem.at[1]),
        pltpu.make_async_copy(moment_hbm, moment, load_sem.at[2]),
        pltpu.make_async_copy(second_hbm, second, load_sem.at[3]),
    ]
    loads[0].start()

    bits = halvings(n_dp)
    nxt, prv = (i + 1) % n_dp, (i + n_dp - 1) % n_dp
    partners = [(flip(i, b), t) for b in bits] + [(nxt, t), (prv, t), (peer, t)]
    for k in range(1, n_t):
        partners += [(i, (t + k) % n_t), (peer, (t + k) % n_t)]
    barrier = pltpu.get_barrier_semaphore()
    for partner in partners:
        pl.semaphore_signal(barrier, inc=1, device_id=partner, device_id_type=MESH)

    mine = pl.ds(t * rows_tok, rows_tok)
    for part in range(2):
        inbox[part, 0, mine, :] = outbox[0, part, 0]
    cold_inbox[mine, :] = cold_outbox[0]

    pl.semaphore_wait(barrier, len(partners))

    def sel_copy(who, part, k):
        return pltpu.make_async_remote_copy(
            src_ref=outbox.at[who, part, k],
            dst_ref=inbox.at[part, who, pl.ds(t * rows_tok, rows_tok)],
            send_sem=sel_send_sem.at[who, part, k],
            recv_sem=sel_recv_sem.at[who, part, k],
            device_id=(i if who == 0 else peer, (t + k) % n_t),
            device_id_type=MESH,
        )

    def cold_sel_copy(k):
        return pltpu.make_async_remote_copy(
            src_ref=cold_outbox.at[k],
            dst_ref=cold_inbox.at[pl.ds(t * rows_tok, rows_tok)],
            send_sem=sel_send_sem.at[0, 2, k],
            recv_sem=sel_recv_sem.at[0, 2, k],
            device_id=(i, (t + k) % n_t),
            device_id_type=MESH,
        )

    sel = {0: [], 1: [], 2: []}
    for part in range(2):
        for k in range(n_t):
            for who in range(2):
                if who or k:
                    sel[part].append(sel_copy(who, part, k))
    for k in range(1, n_t):
        sel[2].append(cold_sel_copy(k))
    og_copy = pltpu.make_async_remote_copy(
        src_ref=og_hbm,
        dst_ref=og.at[pl.ds(tok, tok)],
        send_sem=og_send_sem,
        recv_sem=og_recv_sem,
        device_id=(peer, t),
        device_id_type=MESH,
    )
    for copy in sel[0]:
        copy.start()
    og_copy.start()
    for load in loads[1:]:
        load.start()

    counts = [b // 2 for b in bits]
    offset = [sum(counts[:s]) * unit for s in range(len(bits))]

    def rs_copy(s, q):
        place_ = (pl.ds(offset[s], counts[s] * unit), pl.ds(q * chunk, chunk))
        return pltpu.make_async_remote_copy(
            src_ref=rs_send.at[place_],
            dst_ref=rs_recv.at[place_],
            send_sem=rs_send_sem.at[s, q],
            recv_sem=rs_recv_sem.at[s, q],
            device_id=(flip(i, bits[s]), t),
            device_id_type=MESH,
        )

    tile = min(512, chunk)

    def product(lhs_value_ref, rows, depth, col):
        return jnp.dot(
            lhs_value_ref[rows, :],
            og[pl.ds(0, depth), pl.ds(col, tile)],
            preferred_element_type=F32,
        )

    def wait_sel(part):
        for copy in sel[part]:
            copy.wait_recv()

    wait_sel(0)
    for part in (2, 1):
        for copy in sel[part]:
            copy.start()
    lhs[0, :, pl.ds(0, tok)] = inbox[0, 0].T
    lhs[0, :, pl.ds(tok, tok)] = inbox[0, 1].T
    loads[0].wait()
    og_copy.wait_recv()
    for q in range(CHUNKS):

        @pl.loop(0, chunk // tile)
        def _(n):
            col = pl.multiple_of(q * chunk + n * tile, tile)
            rs_send[pl.ds(0, hw), pl.ds(col, tile)] = product(
                lhs.at[0], slice(None), 2 * tok, col
            ).astype(BF16)

        rs_copy(0, q).start()

    def cold_copy(p, ahead, q):
        slot = p if ahead else p - 1
        place_ = (slot, slice(None), pl.ds(q * chunk, chunk))
        which = 0 if ahead else 1
        return pltpu.make_async_remote_copy(
            src_ref=cold_send.at[p, :, pl.ds(q * chunk, chunk)],
            dst_ref=(prev_out if ahead else next_out).at[place_],
            send_sem=cold_send_sem.at[which, slot, q],
            recv_sem=cold_recv_sem.at[which, slot, q],
            device_id=(nxt if ahead else prv, t),
            device_id_type=MESH,
        )

    wait_sel(2)
    cold_lhs[...] = cold_inbox[...].T
    for q in range(CHUNKS):

        @pl.loop(0, chunk // tile)
        def _(n):
            col = pl.multiple_of(q * chunk + n * tile, tile)
            out = product(cold_lhs, slice(None), tok, col).astype(BF16)
            for p in range(COLD):
                cold_send[p, :, pl.ds(col, tile)] = out[p * BLOCK : (p + 1) * BLOCK]

    def send_cold(q):
        for slot in range(MOSTC):
            cold_copy(slot, True, q).start()
            cold_copy(slot + COLD - MOSTC, False, q).start()

    wait_sel(1)
    lhs[1, :, pl.ds(0, tok)] = inbox[1, 0].T
    lhs[1, :, pl.ds(tok, tok)] = inbox[1, 1].T

    @pl.loop(0, qlocal // tile)
    def _(n):
        col = pl.multiple_of(n * tile, tile)
        acc[:, pl.ds(col, tile)] = product(lhs.at[1], slice(None), 2 * tok, col)

    for load in loads[1:]:
        load.wait()

    def hot_copy(k, q):
        return pltpu.make_async_remote_copy(
            src_ref=hot_send.at[:, pl.ds(q * chunk, chunk)],
            dst_ref=hot_out.at[:, pl.ds(t * qlocal + q * chunk, chunk)],
            send_sem=hot_send_sem.at[k, q],
            recv_sem=hot_recv_sem.at[k, q],
            device_id=(i, (t + k) % n_t),
            device_id_type=MESH,
        )

    def grad_store(q):
        cols = pl.ds(q * chunk, chunk)
        return pltpu.make_async_copy(grad.at[:, cols], grad_out.at[:, cols], out_sem.at[0, q])

    def hot_store(q):
        return pltpu.make_async_copy(
            hot_send.at[:, pl.ds(q * chunk, chunk)],
            hot_out.at[:, pl.ds(t * qlocal + q * chunk, chunk)],
            out_sem.at[1, q],
        )

    step = min(256, chunk)

    def settle(s, q):
        rs_copy(s, q).wait_recv()
        last = s == len(bits) - 1

        @pl.loop(0, chunk // step)
        def _(n):
            cols = pl.ds(pl.multiple_of(q * chunk + n * step, step), step)
            keep = counts[s] * unit
            got = rs_recv[pl.ds(offset[s], keep), cols].astype(F32)
            total = acc[pl.ds(0, keep), cols] + got
            if last:
                grad[:, cols] = total
                new_master, _, _ = adam(total, master[:, cols], moment[:, cols], second[:, cols])
                hot_send[:, cols] = new_master.astype(BF16)
            else:
                sent = counts[s + 1] * unit
                acc[pl.ds(0, sent), cols] = total[:sent]
                rs_send[pl.ds(offset[s + 1], sent), cols] = total[sent:].astype(BF16)

        if last:
            for k in range(1, n_t):
                hot_copy(k, q).start()
            grad_store(q).start()
            hot_store(q).start()
        else:
            rs_copy(s + 1, q).start()

    cold_sent = 0
    for wave in range(CHUNKS + len(bits) - 1):
        for s in reversed(range(len(bits))):
            q = wave - s
            if 0 <= q < CHUNKS:
                settle(s, q)
        if cold_sent < CHUNKS:
            send_cold(cold_sent)
            cold_sent += 1

    for part in range(3):
        for copy in sel[part]:
            copy.wait_send()
    og_copy.wait_send()
    for q in range(CHUNKS):
        for s in range(len(bits)):
            rs_copy(s, q).wait_send()
        grad_store(q).wait()
        hot_store(q).wait()
        for k in range(1, n_t):
            hot_copy(k, q).wait()
        for slot in range(MOSTC):
            cold_copy(slot, True, q).wait()
            cold_copy(slot + COLD - MOSTC, False, q).wait()


def exchange(n_dp, n_t, outbox, cold_outbox, out_grad, master, moment, second):
    tok, qlocal = out_grad.shape
    unit = master.shape[0]
    units = n_dp // 2
    half = max(units // 2, 1)
    stages = max(n_dp.bit_length() - 2, 1)
    traded = (units - 1) * unit
    vmem = pl.BlockSpec(memory_space=pltpu.VMEM)
    anywhere = pl.BlockSpec(memory_space=pl.ANY)
    dma = pltpu.SemaphoreType.DMA
    return pl.pallas_call(
        functools.partial(exchange_kernel, n_dp, n_t),
        out_shape=(
            jax.ShapeDtypeStruct((unit, qlocal), F32),
            jax.ShapeDtypeStruct((unit, qlocal * n_t), BF16),
            jax.ShapeDtypeStruct((MOSTC, BLOCK, qlocal), BF16),
            jax.ShapeDtypeStruct((MOSTC, BLOCK, qlocal), BF16),
        ),
        in_specs=[vmem, vmem] + [anywhere] * 4,
        out_specs=[anywhere] * 4,
        scratch_shapes=[
            pltpu.VMEM((2, 2, tok, half * unit), BF16),
            pltpu.VMEM((tok, COLD * BLOCK), BF16),
            pltpu.VMEM((2 * tok, qlocal), BF16),
            pltpu.VMEM((2, half * unit, 2 * tok), BF16),
            pltpu.VMEM((COLD * BLOCK, tok), BF16),
            pltpu.VMEM((half * unit, qlocal), F32),
            pltpu.VMEM((traded, qlocal), BF16),
            pltpu.VMEM((traded, qlocal), BF16),
            pltpu.VMEM((COLD, BLOCK, qlocal), BF16),
            pltpu.VMEM((unit, qlocal), F32),
            pltpu.VMEM((unit, qlocal), F32),
            pltpu.VMEM((unit, qlocal), F32),
            pltpu.VMEM((unit, qlocal), F32),
            pltpu.VMEM((unit, qlocal), BF16),
            dma((4,)),
            dma((2, 3, n_t)),
            dma((2, 3, n_t)),
            dma(()),
            dma(()),
            dma((stages, CHUNKS)),
            dma((stages, CHUNKS)),
            dma((2, MOSTC, CHUNKS)),
            dma((2, MOSTC, CHUNKS)),
            dma((n_t, CHUNKS)),
            dma((n_t, CHUNKS)),
            dma((2, CHUNKS)),
        ],
        compiler_params=pltpu.CompilerParams(
            collective_id=0, has_side_effects=True, vmem_limit_bytes=60 * 1024 * 1024
        ),
    )(outbox, cold_outbox, out_grad, master, moment, second)


def cold_kernel(where_ref, owner_ref, prev_ref, next_ref, out_ref):
    c = pl.program_id(0)
    from_prev = owner_ref[where_ref[0], c] == 1
    from_next = owner_ref[where_ref[1], c] == 0
    total = jnp.where(from_prev, prev_ref[0].astype(F32), 0.0)
    out_ref[...] = total + jnp.where(from_next, next_ref[0].astype(F32), 0.0)


def ones_before(owner_ref, row, c):
    count = 0
    for b in range(COLD):
        count = count + jnp.where(b < c, owner_ref[row, b], 0)
    return count


def prev_slot(c, n, where_ref, owner_ref):
    return jnp.minimum(ones_before(owner_ref, where_ref[0], c), MOSTC - 1), 0, n


def next_slot(c, n, where_ref, owner_ref):
    row = where_ref[1]
    ones = ones_before(owner_ref, row, COLD)
    place = ones + c - ones_before(owner_ref, row, c)
    return jnp.clip(place - (COLD - MOSTC), 0, MOSTC - 1), 0, n


def merge_cold(where, owner_map, from_prev, from_next):
    qlocal = from_prev.shape[2]
    width = qlocal
    return pl.pallas_call(
        cold_kernel,
        out_shape=jax.ShapeDtypeStruct((COLD * BLOCK, qlocal), F32),
        grid_spec=pltpu.PrefetchScalarGridSpec(
            num_scalar_prefetch=2,
            grid=(COLD, 1),
            in_specs=[
                pl.BlockSpec((1, BLOCK, width), prev_slot),
                pl.BlockSpec((1, BLOCK, width), next_slot),
            ],
            out_specs=pl.BlockSpec((BLOCK, width), lambda c, n, *_: (c, n)),
        ),
    )(where, owner_map, from_prev, from_next)


def per_device(n_dp, n_t, activations, out_grad, block_ids, owner_map, master, moment, second):
    outbox, cold_outbox = gather(n_dp, n_t, master.shape[0], block_ids, owner_map, activations)
    grad, hot_weights, from_prev, from_next = exchange(
        n_dp, n_t, outbox, cold_outbox, out_grad, master, moment, second
    )
    index = lax.axis_index("dp")
    where = jnp.stack([(index + n_dp - 1) % n_dp, (index + 1) % n_dp]).astype(jnp.int32)
    cold_recv = merge_cold(where, owner_map, from_prev, from_next)
    new_master, new_moment, new_second = adam(grad, master, moment, second)
    return (new_master, new_moment, new_second, hot_weights, cold_recv)


def solution(mesh):
    return jax.shard_map(
        functools.partial(per_device, mesh.shape["dp"], mesh.shape["tensor"]),
        mesh=mesh,
        in_specs=(
            P(("dp", "tensor"), None),
            P("dp", "tensor"),
            P(),
            P(),
            P("dp", "tensor"),
            P("dp", "tensor"),
            P("dp", "tensor"),
        ),
        out_specs=(
            P("dp", "tensor"),
            P("dp", "tensor"),
            P("dp", "tensor"),
            P("dp", None),
            P("dp", "tensor"),
        ),
        check_vma=False,
    )
```
